32 devices in a mesh: dp: 8 (over y, x, core), mp: 4 (over z).
Axes of the slice: x: 2, y: 2, z: 4, core: 2. Of those that a mesh axis runs over, the one named last changes fastest.
Arguments:
- tokens: bfloat16 [16384, 1024], P(('dp', 'mp')), may hold values from -6 to 6
- norm_gain: float32 [2, 1024], replicated, may hold values from 0.1 to 1.9
- qkv_weight: bfloat16 [3, 1024, 1024], P(None, 'dp', 'mp')
- out_weight: bfloat16 [1024, 1024], P('mp', 'dp'), may hold values from -0.1875 to 0.1875
- variate_bias: float32 [2, 16], replicated, may hold values from -6 to 6
- ffn_weight: bfloat16 [2, 1024, 2816], P(None, 'dp', 'mp'), may hold values from -0.1875 to 0.1875
- down_weight: bfloat16 [2816, 1024], P('mp', 'dp'), may hold values from -0.109375 to 0.109375
- sample_ids: int32 [16384], P(('dp', 'mp')), may hold values from 0 to 127, as said below
- variate_ids: int32 [16384], P(('dp', 'mp')), may hold values from 0 to 15, as said below
- time_ids: int32 [16384], P(('dp', 'mp')), may hold values from 0 to 31, as said below
Outputs:
- encoded: bfloat16 [16384, 1024], P(('dp', 'mp'))
The draws below stay inside these ranges and needn't reach their ends.
Inputs may be any that keep to these rules, and one draw needn't show every extreme that they name: `sample_ids`: within each packed sequence of 512 tokens the series numbers start at 0 and never fall; a series with v variates (1 to 16) and p patches (4 to 32) holds v * p consecutive tokens, the last series of a sequence may be cut short; some packed sequence holds 128 series of one variate and four patches each. `variate_ids`: A token's offset within its series divided by that series' patch count p. `time_ids`: A token's offset within its series modulo that series' patch count p.
All inputs are finite; a program needn't handle non-finite values.
Results may differ from the reference program's by a relative error of at most 0.017.
Values may be sent and summed in bfloat16 or wider, within the bound.
A program may use at most 128 MiB of HBM per device.

```python
import jax
import jax.numpy as jnp
from jax import lax

D = 1024
HEAD_DIM = 64
HEADS = 16
FF = 2816
L = 512
SEQS = 32
TOKENS = 16384


def packing(key):
    key_var, key_pat, key_pick = jax.random.split(jax.random.fold_in(key, 5), 3)
    slots = L // 4
    variates = jax.random.randint(key_var, (SEQS, slots), 1, 17)
    patches = jax.random.randint(key_pat, (SEQS, slots), 4, 33)
    chosen = jax.random.randint(key_pick, (), 0, SEQS)
    dense = (jnp.arange(SEQS, dtype=jnp.int32) == chosen)[:, None]
    variates = jnp.where(dense, 1, variates)
    patches = jnp.where(dense, 4, patches)
    lengths = variates * patches
    ends = jnp.cumsum(lengths, axis=1)
    starts = ends - lengths
    position = jnp.arange(L, dtype=jnp.int32)
    series = jnp.sum((position[None, :, None] >= ends[:, None, :]).astype(jnp.int32), axis=2)
    begin = jnp.take_along_axis(starts, series, axis=1)
    span = jnp.take_along_axis(patches, series, axis=1)
    offset = position[None, :] - begin
    return (series.reshape(-1).astype(jnp.int32), (offset // span).reshape(-1).astype(jnp.int32), (offset % span).reshape(-1).astype(jnp.int32))


def draw_sample_ids(key, part):
    return packing(key)[0]


def draw_variate_ids(key, part):
    return packing(key)[1]


def draw_time_ids(key, part):
    return packing(key)[2]


def draw_qkv_weight(key, part):
    key_base = jax.random.fold_in(jax.random.fold_in(key, 11), 0)
    base = jax.random.normal(key_base, (3, D, D), jnp.float32) * D ** (-0.5)
    return base.astype(jnp.bfloat16)


def shard_levels(stream_key, extent, shards, least, top_value):
    level, own = 1.0, jax.random.fold_in(stream_key, 6)
    for dim, shards_of in shards:
        heights = jnp.exp(jax.random.uniform(jax.random.fold_in(own, dim), (shards_of,), jnp.float32, least / len(shards), top_value / len(shards)))
        level = level * jnp.repeat(heights, extent[dim] // shards_of).reshape([-1 if axis == dim else 1 for axis in range(len(extent))])
    return level


def gaussian(stream_key, dims, spread, most, pieces=(), held_as=jnp.bfloat16):
    level = shard_levels(stream_key, dims, pieces, -0.22, 0.18) if pieces else 1.0
    entries = jax.random.normal(stream_key, dims, jnp.float32) * spread * level
    return jnp.minimum(jnp.maximum(entries, -most), most).astype(held_as)


def setup_inputs(seed: int = 0) -> dict:
    keys = jax.random.split(jax.random.key(seed), 11)
    tokens = gaussian(keys[0], (TOKENS, D), 1.0, 6.0, ((0, 32),))
    norm_gain = jnp.clip(1.0 + 0.18 * jax.random.normal(keys[1], (2, D), jnp.float32), 0.1, 1.9)
    qkv_weight = draw_qkv_weight(jax.random.fold_in(keys[10], 71), 0)
    out_weight = gaussian(keys[3], (D, D), D ** -0.5, 0.1875, ((0, 4), (1, 8)))
    variate_bias = gaussian(keys[4], (2, HEADS), 1.5, 6.0, (), jnp.float32)
    ffn_weight = gaussian(keys[5], (2, D, FF), D ** -0.5, 0.1875, ((1, 8), (2, 4)))
    down_weight = gaussian(keys[6], (FF, D), FF ** -0.5, 0.109375, ((0, 4), (1, 8)))
    sample_ids = draw_sample_ids(jax.random.fold_in(keys[10], 71), 0)
    variate_ids = draw_variate_ids(jax.random.fold_in(keys[10], 71), 0)
    time_ids = draw_time_ids(jax.random.fold_in(keys[10], 71), 0)
    return dict(tokens=tokens, norm_gain=norm_gain, qkv_weight=qkv_weight, out_weight=out_weight, variate_bias=variate_bias, ffn_weight=ffn_weight, down_weight=down_weight, sample_ids=sample_ids, variate_ids=variate_ids, time_ids=time_ids)


def rms_norm(values, gain):
    wide = values.astype(jnp.float32)
    square = lax.optimization_barrier(jnp.mean(wide * wide, axis=-1, keepdims=True))
    return (wide * lax.rsqrt(square + 1e-05) * gain[None, :]).astype(jnp.bfloat16)

def rotate(values, times):
    half = values.shape[-1] // 2
    freq = 10000.0 ** (-jnp.arange(half, dtype=jnp.float32) / half)
    angle = times.astype(jnp.float32)[:, None] * freq[None, :]
    cosine = jnp.cos(angle)[:, None, :]
    sine = jnp.sin(angle)[:, None, :]
    first = values[..., :half]
    second = values[..., half:]
    return jnp.concatenate([first * cosine - second * sine, first * sine + second * cosine], axis=-1)

def reference(tokens, norm_gain, qkv_weight, out_weight, variate_bias, ffn_weight, down_weight, sample_ids, variate_ids, time_ids):
    total = tokens.shape[0]
    first_normed = rms_norm(tokens, norm_gain[0])
    query_raw = jnp.dot(first_normed, qkv_weight[0], preferred_element_type=jnp.float32)
    key_raw = jnp.dot(first_normed, qkv_weight[1], preferred_element_type=jnp.float32)
    value_raw = jnp.dot(first_normed, qkv_weight[2], preferred_element_type=jnp.float32)
    queries = rotate(query_raw.reshape(total, HEADS, HEAD_DIM), time_ids).astype(jnp.bfloat16)
    keys_rot = rotate(key_raw.reshape(total, HEADS, HEAD_DIM), time_ids).astype(jnp.bfloat16)
    values = value_raw.reshape(total, HEADS, HEAD_DIM).astype(jnp.bfloat16)
    count = total // L

    def one_sequence(args):
        qs, ks, vs, samples, variates = args
        scores = jnp.einsum('qhd,khd->hqk', qs.astype(jnp.float32), ks.astype(jnp.float32)) * HEAD_DIM ** (-0.5)
        same = variates[:, None] == variates[None, :]
        scores = scores + jnp.where(same[None], variate_bias[0][:, None, None], variate_bias[1][:, None, None])
        scores = jnp.where((samples[:, None] == samples[None, :])[None], scores, -1e+30)
        top = lax.optimization_barrier(jnp.max(scores, axis=2, keepdims=True))
        expo = jnp.exp(scores - top)
        weights = (expo / lax.optimization_barrier(jnp.sum(expo, axis=2, keepdims=True))).astype(jnp.bfloat16)
        return jnp.einsum('hqk,khd->qhd', weights.astype(jnp.float32), vs.astype(jnp.float32)).astype(jnp.bfloat16)
    attended = lax.map(one_sequence, (queries.reshape(count, L, HEADS, HEAD_DIM), keys_rot.reshape(count, L, HEADS, HEAD_DIM), values.reshape(count, L, HEADS, HEAD_DIM), sample_ids.reshape(count, L), variate_ids.reshape(count, L)))
    attended = attended.reshape(total, D)
    residual = (tokens.astype(jnp.float32) + jnp.dot(attended, out_weight, preferred_element_type=jnp.float32)).astype(jnp.bfloat16)
    second_normed = rms_norm(residual, norm_gain[1])
    gate = jnp.dot(second_normed, ffn_weight[0], preferred_element_type=jnp.float32)
    up = jnp.dot(second_normed, ffn_weight[1], preferred_element_type=jnp.float32)
    hidden = (jax.nn.silu(gate) * up).astype(jnp.bfloat16)
    return (residual.astype(jnp.float32) + jnp.dot(hidden, down_weight, preferred_element_type=jnp.float32)).astype(jnp.bfloat16)
```

```python
import jax
import jax.numpy as jnp
from jax import lax
from jax.sharding import PartitionSpec as P

HEAD_DIM = 64
L = 512


def rms_norm(values, gain):
    wide = values.astype(jnp.float32)
    square = jnp.mean(wide * wide, axis=-1, keepdims=True)
    return (wide * lax.rsqrt(square + 1e-05) * gain[None, :]).astype(jnp.bfloat16)


def rotate(values, times):
    half = values.shape[-1] // 2
    freq = 10000.0 ** (-jnp.arange(half, dtype=jnp.float32) / half)
    angle = times.astype(jnp.float32)[:, None] * freq[None, :]
    cosine = jnp.cos(angle)[:, None, :]
    sine = jnp.sin(angle)[:, None, :]
    first = values[..., :half]
    second = values[..., half:]
    return jnp.concatenate(
        [first * cosine - second * sine, first * sine + second * cosine], axis=-1
    )


def rotated(raw, times):
    row_total, local_width = raw.shape
    turned = rotate(raw.reshape(row_total, local_width // HEAD_DIM, HEAD_DIM), times)
    return turned.reshape(row_total, local_width).astype(jnp.bfloat16)


def attend(queries, keys_rot, values, samples, variates, bias):
    row_total, local_width = queries.shape
    heads_here = local_width // HEAD_DIM
    count = row_total // L

    def one_sequence(args):
        qs, ks, vs, sample_row, variate_row = args
        scores = jnp.einsum(
            "qhd,khd->hqk", qs, ks, preferred_element_type=jnp.float32
        ) * HEAD_DIM ** (-0.5)
        same = variate_row[:, None] == variate_row[None, :]
        scores = scores + jnp.where(same[None], bias[0][:, None, None], bias[1][:, None, None])
        scores = jnp.where((sample_row[:, None] == sample_row[None, :])[None], scores, -1e30)
        top = jnp.max(scores, axis=2, keepdims=True)
        expo = jnp.exp(scores - top)
        weights = (expo / jnp.sum(expo, axis=2, keepdims=True)).astype(jnp.bfloat16)
        return jnp.einsum("hqk,khd->qhd", weights, vs, preferred_element_type=jnp.float32).astype(
            jnp.bfloat16
        )

    shape = (count, L, heads_here, HEAD_DIM)
    result = lax.map(
        one_sequence,
        (
            queries.reshape(shape),
            keys_rot.reshape(shape),
            values.reshape(shape),
            samples.reshape(count, L),
            variates.reshape(count, L),
        ),
    )
    return result.reshape(row_total, local_width)


def local(
    tokens,
    norm_gain,
    qkv_weight,
    out_weight,
    variate_bias,
    ffn_weight,
    down_weight,
    sample_ids,
    variate_ids,
    time_ids,
):
    first_normed = rms_norm(tokens, norm_gain[0])
    wide_columns = lax.all_gather(qkv_weight, "mp", axis=2, tiled=True)
    columns = first_normed
    projected = jnp.einsum(
        "rc,jcd->jrd",
        columns,
        lax.all_gather(wide_columns, "dp", axis=1, tiled=True),
        preferred_element_type=jnp.float32,
    )
    queries = rotated(projected[0], time_ids)
    keys_rot = rotated(projected[1], time_ids)
    values = projected[2].astype(jnp.bfloat16)
    back_rows = attend(queries, keys_rot, values, sample_ids, variate_ids, variate_bias)
    out_rows = lax.all_gather(out_weight, "mp", axis=0, tiled=True)
    mixed = jnp.dot(
        back_rows,
        lax.all_gather(out_rows, "dp", axis=1, tiled=True),
        preferred_element_type=jnp.float32,
    )
    residual = (tokens.astype(jnp.float32) + mixed).astype(jnp.bfloat16)
    second_normed = rms_norm(residual, norm_gain[1])
    ffn_columns = lax.all_gather(ffn_weight, "mp", axis=2, tiled=True)
    columns = second_normed
    gate_up = jnp.einsum(
        "rc,jcf->jrf",
        columns,
        lax.all_gather(ffn_columns, "dp", axis=1, tiled=True),
        preferred_element_type=jnp.float32,
    )
    hidden = (jax.nn.silu(gate_up[0]) * gate_up[1]).astype(jnp.bfloat16)
    down_full = lax.all_gather(down_weight, "mp", axis=0, tiled=True)
    feed = jnp.dot(
        hidden,
        lax.all_gather(down_full, "dp", axis=1, tiled=True),
        preferred_element_type=jnp.float32,
    )
    return (residual.astype(jnp.float32) + feed).astype(jnp.bfloat16)


def solution(mesh):
    return jax.shard_map(
        local,
        mesh=mesh,
        in_specs=(
            P(("dp", "mp"), None),
            P(),
            P(None, "dp", "mp"),
            P("mp", "dp"),
            P(),
            P(None, "dp", "mp"),
            P("mp", "dp"),
            P(("dp", "mp")),
            P(("dp", "mp")),
            P(("dp", "mp")),
        ),
        out_specs=P(("dp", "mp"), None),
        check_vma=False,
    )
```

```python
import functools
import math

import jax
import jax.numpy as jnp
from jax import lax
from jax.experimental import pallas as pl
from jax.experimental.pallas import tpu as pltpu
from jax.sharding import PartitionSpec as P

HEAD_DIM = 64
L = 512


def rms_norm(values, gain):
    wide = values.astype(jnp.float32)
    square = jnp.mean(wide * wide, axis=-1, keepdims=True)
    return (wide * lax.rsqrt(square + 1e-05) * gain[None, :]).astype(jnp.bfloat16)


def rotate(values, times):
    half = values.shape[-1] // 2
    freq = 10000.0 ** (-jnp.arange(half, dtype=jnp.float32) / half)
    angle = times.astype(jnp.float32)[:, None] * freq[None, :]
    cosine = jnp.cos(angle)[:, None, :]
    sine = jnp.sin(angle)[:, None, :]
    first = values[..., :half]
    second = values[..., half:]
    return jnp.concatenate(
        [first * cosine - second * sine, first * sine + second * cosine], axis=-1
    )


def rotated(raw, times):
    row_total, local_width = raw.shape
    turned = rotate(raw.reshape(row_total, local_width // HEAD_DIM, HEAD_DIM), times)
    return turned.reshape(row_total, local_width).astype(jnp.bfloat16)


def attend(queries, keys_rot, values, samples, variates, bias):
    row_total, local_width = queries.shape
    heads_here = local_width // HEAD_DIM
    count = row_total // L

    def one_sequence(args):
        qs, ks, vs, sample_row, variate_row = args
        scores = jnp.einsum(
            "qhd,khd->hqk", qs, ks, preferred_element_type=jnp.float32
        ) * HEAD_DIM ** (-0.5)
        same = variate_row[:, None] == variate_row[None, :]
        scores = scores + jnp.where(same[None], bias[0][:, None, None], bias[1][:, None, None])
        scores = jnp.where((sample_row[:, None] == sample_row[None, :])[None], scores, -1e30)
        top = jnp.max(scores, axis=2, keepdims=True)
        expo = jnp.exp(scores - top)
        weights = (expo / jnp.sum(expo, axis=2, keepdims=True)).astype(jnp.bfloat16)
        return jnp.einsum("hqk,khd->qhd", weights, vs, preferred_element_type=jnp.float32).astype(
            jnp.bfloat16
        )

    shape = (count, L, heads_here, HEAD_DIM)
    result = lax.map(
        one_sequence,
        (
            queries.reshape(shape),
            keys_rot.reshape(shape),
            values.reshape(shape),
            samples.reshape(count, L),
            variates.reshape(count, L),
        ),
    )
    return result.reshape(row_total, local_width)


def local(
    tokens,
    norm_gain,
    qkv_weight,
    out_weight,
    variate_bias,
    ffn_weight,
    down_weight,
    sample_ids,
    variate_ids,
    time_ids,
):
    first_normed = rms_norm(tokens, norm_gain[0])
    wide_columns = lax.all_gather(qkv_weight, "mp", axis=2, tiled=True)
    columns = first_normed
    projected = jnp.einsum(
        "rc,jcd->jrd",
        columns,
        lax.all_gather(wide_columns, "dp", axis=1, tiled=True),
        preferred_element_type=jnp.float32,
    )
    queries = rotated(projected[0], time_ids)
    keys_rot = rotated(projected[1], time_ids)
    values = projected[2].astype(jnp.bfloat16)
    back_rows = attend(queries, keys_rot, values, sample_ids, variate_ids, variate_bias)
    out_rows = lax.all_gather(out_weight, "mp", axis=0, tiled=True)
    mixed = jnp.dot(
        back_rows,
        lax.all_gather(out_rows, "dp", axis=1, tiled=True),
        preferred_element_type=jnp.float32,
    )
    residual = (tokens.astype(jnp.float32) + mixed).astype(jnp.bfloat16)
    second_normed = rms_norm(residual, norm_gain[1])
    ffn_columns = lax.all_gather(ffn_weight, "mp", axis=2, tiled=True)
    columns = second_normed
    gate_up = jnp.einsum(
        "rc,jcf->jrf",
        columns,
        lax.all_gather(ffn_columns, "dp", axis=1, tiled=True),
        preferred_element_type=jnp.float32,
    )
    hidden = (jax.nn.silu(gate_up[0]) * gate_up[1]).astype(jnp.bfloat16)
    down_full = lax.all_gather(down_weight, "mp", axis=0, tiled=True)
    feed = jnp.dot(
        hidden,
        lax.all_gather(down_full, "dp", axis=1, tiled=True),
        preferred_element_type=jnp.float32,
    )
    return (residual.astype(jnp.float32) + feed).astype(jnp.bfloat16)

MESH = pl.DeviceIdType.MESH
PIECES = 4
ROWS = 256
WIDE = 2 * HEAD_DIM


def event_order(spans):
    due = []
    start = 0.0
    for which, span in enumerate(spans):
        begin = max(0.0, start - 0.12 * sum(spans))
        for stage, part in enumerate((0.0, 0.15, 0.3, 0.55, 0.8, 1.0)):
            due.append((begin + part * 1.3 * span, which, stage))
        start += span
    return [(which, stage) for _, which, stage in sorted(due)]


def layer_kernel(
    ring, spans,
    bias_ref, tokens_ref, gain_ref, ids_ref, qkv_in, out_in, ffn_in, down_in,
    final_ref,
    qkv_buf, out_buf, gate_buf, up_buf, down_buf,
    normed, queries, keys, values, attended, residual, gates, hidden, cosine, sine, columns,
    send_sem, recv_sem, local_sem,
):
    bufs = (qkv_buf, out_buf, gate_buf, up_buf, down_buf)
    dp = lax.axis_index("dp")
    z = lax.axis_index("mp")
    core = lax.rem(dp, 2)
    x = lax.rem(dp // 2, 2)
    y = dp // 4
    up_z = lax.rem(z + 1, ring)
    down_z = lax.rem(z + ring - 1, ring)
    whole = slice(None)
    to_x = {"dp": (y * 2 + 1 - x) * 2 + core, "mp": z}
    to_y = {"dp": ((1 - y) * 2 + x) * 2 + core, "mp": z}
    to_core = {"dp": (y * 2 + x) * 2 + 1 - core, "mp": z}
    to_up = {"dp": dp, "mp": up_z}
    to_down = {"dp": dp, "mp": down_z}

    def target(piece, hop):
        mirrored = piece % 2 == 1
        if hop == 0:
            return to_up
        if hop == 1:
            return to_down
        if hop == 2:
            return to_down if mirrored else to_up
        if hop == 3:
            return to_y if mirrored else to_x
        if hop == 4:
            return to_x if mirrored else to_y
        return to_core

    def region(piece, hop):
        mirrored = piece % 2 == 1
        behind = up_z if mirrored else down_z
        pair = (whole, x) if mirrored else (y, whole)
        if hop == 5:
            return (whole, whole, core, whole)
        if piece < 2:
            return {
                0: (y, x, core, z), 1: (y, x, core, z), 2: (y, x, core, behind),
                3: (y, x, core, whole), 4: pair + (core, whole),
            }[hop]
        return {
            3: (y, x, core, z), 4: pair + (core, z), 0: (whole, whole, core, z),
            1: (whole, whole, core, z), 2: (whole, whole, core, behind),
        }[hop]

    def copy(which, piece, hop):
        part = bufs[which].at[region(piece, hop) + (whole, piece)]
        slot = (which * PIECES + piece) * 6 + hop
        return pltpu.make_async_remote_copy(
            src_ref=part, dst_ref=part, send_sem=send_sem.at[slot], recv_sem=recv_sem.at[slot],
            device_id=target(piece, hop), device_id_type=MESH,
        )

    def own(which):
        source = (qkv_in, out_in, ffn_in.at[pl.ds(0, 1)], ffn_in.at[pl.ds(1, 1)], down_in)[which]
        return pltpu.make_async_copy(source, bufs[which].at[y, x, core, z], local_sem.at[which])

    def event(which, stage):
        for piece in range(PIECES):
            early = piece < 2
            first, second = (1, 0) if piece % 2 else (0, 1)
            waits, sends = (
                (((), (0, 1)), ((first,), (2,)), ((second, 2), (3,)), ((3,), (4,)), ((4,), (5,)), ((5,), ()))
                if early else
                (((), (3,)), ((3,), (4,)), ((4,), (0, 1)), ((first,), (2,)), ((second, 2), (5,)), ((5,), ()))
            )[stage]
            for hop in waits:
                copy(which, piece, hop).wait_recv()
            for hop in sends:
                copy(which, piece, hop).start()

    order = event_order(spans)
    cursor = [0]

    def take(count):
        picked = order[cursor[0]:cursor[0] + count]
        cursor[0] += len(picked)
        return picked

    def until(which):
        return take(order.index((which, 5)) + 1 - cursor[0])

    def at_steps(total, picked):
        plan = [[] for _ in range(total)]
        for place, item in enumerate(picked):
            plan[place * total // len(picked)].append(item)

        def run(step):
            for place, items in enumerate(plan):
                if items:
                    @pl.when(step == place)
                    def _():
                        for item in items:
                            event(*item)
        return run

    for which in range(len(bufs)):
        own(which).start()
    barrier = pltpu.get_barrier_semaphore()
    for peer in (to_x, to_y, to_core, to_up, to_down):
        pl.semaphore_signal(barrier, inc=1, device_id=peer, device_id_type=MESH)
    pl.semaphore_wait(barrier, 5)
    for which in range(len(bufs)):
        own(which).wait()

    first_wave = until(0)
    cut = min(3, len(first_wave))
    for item in first_wave[:cut]:
        event(*item)

    total_rows, width = tokens_ref.shape
    blocks = total_rows // ROWS

    def norm_rows(source, gain_row):
        gain = gain_ref[gain_row:gain_row + 1, :]

        def body(step, carry):
            rows = pl.ds(pl.multiple_of(step * 128, 128), 128)
            wide = source[rows, :].astype(jnp.float32)
            square = jnp.mean(wide * wide, axis=-1, keepdims=True)
            normed[rows, :] = (wide * lax.rsqrt(square + 1e-05) * gain).astype(jnp.bfloat16)
            return carry
        lax.fori_loop(0, total_rows // 128, body, 0)

    norm_rows(tokens_ref, 0)
    ids = ids_ref[...].astype(jnp.float32)
    times = jnp.broadcast_to(ids[2:3, :], (WIDE, total_rows)).T
    columns[0] = jnp.broadcast_to(ids[0:1, :], (WIDE, total_rows)).T
    columns[1] = jnp.broadcast_to(ids[1:2, :], (WIDE, total_rows)).T
    half = HEAD_DIM // 2
    lane = lax.broadcasted_iota(jnp.int32, (1, WIDE), 1)
    slot_in_half = lax.rem(lane, half).astype(jnp.float32)
    freq = jnp.exp(slot_in_half * (-math.log(10000.0) / half))
    front = lax.rem(lane, HEAD_DIM) < half
    angle = times * freq
    cosine[...] = jnp.cos(angle)
    sine[...] = jnp.where(front, -1.0, 1.0) * jnp.sin(angle)

    for item in first_wave[cut:]:
        event(*item)

    def rotated_wide(raw):
        swapped = jnp.where(front, pltpu.roll(raw, WIDE - half, 1), pltpu.roll(raw, half, 1))
        return raw * cosine[...] + swapped * sine[...]

    later = until(2)
    early_count = min(len(later), 3)
    project_events = at_steps(ring, later[:early_count])
    attend_steps = (width // WIDE) * blocks
    attend_events = at_steps(attend_steps, later[early_count:])

    def project(step, carry):
        def product(kind):
            shape = (width, qkv_buf.shape[-1])
            weight = qkv_buf[:, :, :, step, kind].reshape(shape)
            return jnp.dot(normed[...], weight, preferred_element_type=jnp.float32)
        groups = qkv_buf.shape[-1] // WIDE
        for kind, held in enumerate((queries, keys, values)):
            raw = product(kind)
            for group in range(groups):
                part = raw[:, group * WIDE:(group + 1) * WIDE]
                if kind < 2:
                    part = rotated_wide(part)
                part = part.astype(jnp.bfloat16)
                if kind == 0:
                    part = part * jnp.bfloat16(HEAD_DIM ** -0.5)
                held[step * groups + group] = part
        project_events(step)
        return carry
    lax.fori_loop(0, ring, project, 0)

    left = lane < HEAD_DIM

    def attend_step(step, carry):
        pair = step // blocks
        block = lax.rem(step, blocks)
        rows = pl.ds(pl.multiple_of(block * ROWS, ROWS), ROWS)
        base = pl.multiple_of((block * ROWS) // L * L, L)
        span = pl.ds(base, L)
        same_series = columns[0, rows, 0:1] == ids_ref[0:1, span].astype(jnp.float32)
        same_variate = columns[1, rows, 0:1] == ids_ref[1:2, span].astype(jnp.float32)
        both = queries[pair, rows, :]
        key_rows = keys[pair, span, :]
        value_rows = values[pair, span, :]
        results = []
        for side in range(2):
            head = pair * 2 + side
            chosen = left if side == 0 else jnp.logical_not(left)
            mine = both * chosen.astype(jnp.bfloat16)
            scores = lax.dot_general(
                mine, key_rows, (((1,), (1,)), ((), ())), preferred_element_type=jnp.float32
            )
            scores = scores + jnp.where(same_variate, bias_ref[0, head], bias_ref[1, head])
            scores = jnp.where(same_series, scores, -1e30)
            top = jnp.max(scores, axis=1, keepdims=True)
            expo = jnp.exp(scores - top)
            total = jnp.sum(expo, axis=1, keepdims=True)
            mixed = jnp.dot(
                expo.astype(jnp.bfloat16), value_rows, preferred_element_type=jnp.float32
            )
            results.append(mixed / total)
        lanes = pl.ds(pl.multiple_of(pair * WIDE, WIDE), WIDE)
        attended[rows, lanes] = jnp.where(left, results[0], results[1]).astype(jnp.bfloat16)
        attend_events(step)
        return carry
    lax.fori_loop(0, attend_steps, attend_step, 0)

    def block_pair(buf, side_y, side_x, index):
        return jnp.concatenate(
            [buf[side_y, side_x, half_core, index].reshape(-1, buf.shape[-1]) for half_core in range(2)],
            axis=1,
        )

    slab = 2 * out_buf.shape[-1]

    def out_step(step, carry):
        lanes = pl.ds(pl.multiple_of(step * slab, slab), slab)
        weight = block_pair(out_buf, step // 2, lax.rem(step, 2), whole)
        mixed = jnp.dot(attended[...], weight, preferred_element_type=jnp.float32)
        residual[:, lanes] = (tokens_ref[:, lanes].astype(jnp.float32) + mixed).astype(jnp.bfloat16)
        return carry
    lax.fori_loop(0, 4, out_step, 0)
    norm_rows(residual, 1)

    gate_events = at_steps(ring, until(3))

    def gate_step(step, carry):
        weight = gate_buf[:, :, :, step].reshape(width, gate_buf.shape[-1])
        gates[step] = jnp.dot(normed[...], weight, preferred_element_type=jnp.float32)
        gate_events(step)
        return carry
    lax.fori_loop(0, ring, gate_step, 0)

    up_events = at_steps(ring, until(4))

    def up_step(step, carry):
        weight = up_buf[:, :, :, step].reshape(width, up_buf.shape[-1])
        up = jnp.dot(normed[...], weight, preferred_element_type=jnp.float32)
        gate = gates[step]
        hidden[step] = (gate / (1.0 + jnp.exp(-gate)) * up).astype(jnp.bfloat16)
        up_events(step)
        return carry
    lax.fori_loop(0, ring, up_step, 0)

    def down_step(step, carry):
        lanes = pl.ds(pl.multiple_of(step * slab, slab), slab)
        total = residual[:, lanes].astype(jnp.float32)
        for index in range(ring):
            weight = block_pair(down_buf, step // 2, lax.rem(step, 2), index)
            total = total + jnp.dot(hidden[index], weight, preferred_element_type=jnp.float32)
        final_ref[:, lanes] = total.astype(jnp.bfloat16)
        return carry
    lax.fori_loop(0, 4, down_step, 0)

    def drain(which, piece, hop):
        copy(which, piece, hop).wait_send()
    for which in range(len(bufs)):
        for piece in range(PIECES):
            for hop in range(6):
                drain(which, piece, hop)


def fused(
    ring, tokens, norm_gain, qkv_weight, out_weight, variate_bias, ffn_weight, down_weight,
    sample_ids, variate_ids, time_ids,
):
    rows, width = tokens.shape
    ids = jnp.stack([sample_ids, variate_ids, time_ids])
    qkv = qkv_weight.reshape(qkv_weight.shape[0], PIECES, -1, qkv_weight.shape[2])
    out = out_weight.reshape(1, PIECES, -1, out_weight.shape[1])
    ffn = ffn_weight.reshape(2, PIECES, -1, ffn_weight.shape[2])
    down = down_weight.reshape(1, PIECES, -1, down_weight.shape[1])
    spans = tuple(float(n) for n in (qkv.size, out.size, ffn.size // 2, ffn.size // 2, down.size))
    shapes = (qkv.shape, out.shape, (1,) + ffn.shape[1:], (1,) + ffn.shape[1:], down.shape)
    buffers = [pltpu.VMEM((2, 2, 2, ring) + shape, jnp.bfloat16) for shape in shapes]
    pairs = width // WIDE
    per_pair = pltpu.VMEM((pairs, rows, WIDE), jnp.bfloat16)
    flat = pltpu.VMEM((rows, width), jnp.bfloat16)
    vmem = pl.BlockSpec(memory_space=pltpu.VMEM)
    anywhere = pl.BlockSpec(memory_space=pl.ANY)
    copies = len(shapes) * PIECES * 6
    return pl.pallas_call(
        functools.partial(layer_kernel, ring, spans),
        out_shape=jax.ShapeDtypeStruct((rows, width), jnp.bfloat16),
        in_specs=[pl.BlockSpec(memory_space=pltpu.SMEM), vmem, vmem, vmem] + [anywhere] * 4,
        out_specs=vmem,
        scratch_shapes=buffers + [
            flat, per_pair, per_pair, per_pair, flat, flat,
            pltpu.VMEM((ring, rows, ffn.shape[-1]), jnp.float32),
            pltpu.VMEM((ring, rows, ffn.shape[-1]), jnp.bfloat16),
            pltpu.VMEM((rows, WIDE), jnp.float32),
            pltpu.VMEM((rows, WIDE), jnp.float32),
            pltpu.VMEM((2, rows, WIDE), jnp.float32),
            pltpu.SemaphoreType.DMA((copies,)),
            pltpu.SemaphoreType.DMA((copies,)),
            pltpu.SemaphoreType.DMA((len(shapes),)),
        ],
        compiler_params=pltpu.CompilerParams(
            collective_id=0, has_side_effects=True, vmem_limit_bytes=60 * 1024 * 1024
        ),
    )(variate_bias, tokens, norm_gain, ids, qkv, out, ffn, down)


def solution(mesh):
    ring = mesh.shape["mp"]
    body = functools.partial(fused, ring) if (mesh.shape["dp"], ring) == (2 ** 3, 2 ** 2) else local
    return jax.shard_map(
        body,
        mesh=mesh,
        in_specs=(
            P(("dp", "mp"), None),
            P(),
            P(None, "dp", "mp"),
            P("mp", "dp"),
            P(),
            P(None, "dp", "mp"),
            P("mp", "dp"),
            P(("dp", "mp")),
            P(("dp", "mp")),
            P(("dp", "mp")),
        ),
        out_specs=P(("dp", "mp"), None),
        check_vma=False,
    )
```

```python
import functools
import math

import jax
import jax.numpy as jnp
from jax import lax
from jax.experimental import pallas as pl
from jax.experimental.pallas import tpu as pltpu
from jax.sharding import PartitionSpec as P

HEAD_DIM = 64
L = 512


def rms_norm(values, gain):
    wide = values.astype(jnp.float32)
    square = jnp.mean(wide * wide, axis=-1, keepdims=True)
    return (wide * lax.rsqrt(square + 1e-05) * gain[None, :]).astype(jnp.bfloat16)


def rotate(values, times):
    half = values.shape[-1] // 2
    freq = 10000.0 ** (-jnp.arange(half, dtype=jnp.float32) / half)
    angle = times.astype(jnp.float32)[:, None] * freq[None, :]
    cosine = jnp.cos(angle)[:, None, :]
    sine = jnp.sin(angle)[:, None, :]
    first = values[..., :half]
    second = values[..., half:]
    return jnp.concatenate(
        [first * cosine - second * sine, first * sine + second * cosine], axis=-1
    )


def rotated(raw, times):
    row_total, local_width = raw.shape
    turned = rotate(raw.reshape(row_total, local_width // HEAD_DIM, HEAD_DIM), times)
    return turned.reshape(row_total, local_width).astype(jnp.bfloat16)


def attend(queries, keys_rot, values, samples, variates, bias):
    row_total, local_width = queries.shape
    heads_here = local_width // HEAD_DIM
    count = row_total // L

    def one_sequence(args):
        qs, ks, vs, sample_row, variate_row = args
        scores = jnp.einsum(
            "qhd,khd->hqk", qs, ks, preferred_element_type=jnp.float32
        ) * HEAD_DIM ** (-0.5)
        same = variate_row[:, None] == variate_row[None, :]
        scores = scores + jnp.where(same[None], bias[0][:, None, None], bias[1][:, None, None])
        scores = jnp.where((sample_row[:, None] == sample_row[None, :])[None], scores, -1e30)
        top = jnp.max(scores, axis=2, keepdims=True)
        expo = jnp.exp(scores - top)
        weights = (expo / jnp.sum(expo, axis=2, keepdims=True)).astype(jnp.bfloat16)
        return jnp.einsum("hqk,khd->qhd", weights, vs, preferred_element_type=jnp.float32).astype(
            jnp.bfloat16
        )

    shape = (count, L, heads_here, HEAD_DIM)
    result = lax.map(
        one_sequence,
        (
            queries.reshape(shape),
            keys_rot.reshape(shape),
            values.reshape(shape),
            samples.reshape(count, L),
            variates.reshape(count, L),
        ),
    )
    return result.reshape(row_total, local_width)


def local(
    tokens,
    norm_gain,
    qkv_weight,
    out_weight,
    variate_bias,
    ffn_weight,
    down_weight,
    sample_ids,
    variate_ids,
    time_ids,
):
    first_normed = rms_norm(tokens, norm_gain[0])
    wide_columns = lax.all_gather(qkv_weight, "mp", axis=2, tiled=True)
    columns = first_normed
    projected = jnp.einsum(
        "rc,jcd->jrd",
        columns,
        lax.all_gather(wide_columns, "dp", axis=1, tiled=True),
        preferred_element_type=jnp.float32,
    )
    queries = rotated(projected[0], time_ids)
    keys_rot = rotated(projected[1], time_ids)
    values = projected[2].astype(jnp.bfloat16)
    back_rows = attend(queries, keys_rot, values, sample_ids, variate_ids, variate_bias)
    out_rows = lax.all_gather(out_weight, "mp", axis=0, tiled=True)
    mixed = jnp.dot(
        back_rows,
        lax.all_gather(out_rows, "dp", axis=1, tiled=True),
        preferred_element_type=jnp.float32,
    )
    residual = (tokens.astype(jnp.float32) + mixed).astype(jnp.bfloat16)
    second_normed = rms_norm(residual, norm_gain[1])
    ffn_columns = lax.all_gather(ffn_weight, "mp", axis=2, tiled=True)
    columns = second_normed
    gate_up = jnp.einsum(
        "rc,jcf->jrf",
        columns,
        lax.all_gather(ffn_columns, "dp", axis=1, tiled=True),
        preferred_element_type=jnp.float32,
    )
    hidden = (jax.nn.silu(gate_up[0]) * gate_up[1]).astype(jnp.bfloat16)
    down_full = lax.all_gather(down_weight, "mp", axis=0, tiled=True)
    feed = jnp.dot(
        hidden,
        lax.all_gather(down_full, "dp", axis=1, tiled=True),
        preferred_element_type=jnp.float32,
    )
    return (residual.astype(jnp.float32) + feed).astype(jnp.bfloat16)

MESH = pl.DeviceIdType.MESH
PIECES = 4
ROWS = 256
WIDE = 2 * HEAD_DIM
STAGES = 7
ARRAY_TURNS = 1.5
LATE_TURNS = 1.2


def event_order(arrays):
    due = []
    for which in range(arrays):
        for stage in range(STAGES):
            for late in range(2):
                due.append((which * ARRAY_TURNS + stage + late * LATE_TURNS, which, stage, late))
    return [item[1:] for item in sorted(due)]


def layer_kernel(
    ring,
    bias_ref, tokens_ref, gain_ref, ids_ref, qkv_in, out_in, ffn_in, down_in,
    final_ref,
    qkv_buf, out_buf, gate_buf, up_buf, down_buf,
    normed, queries, keys, values, attended, residual, gates, hidden, cosine, sine, columns,
    send_sem, recv_sem, local_sem,
):
    bufs = (qkv_buf, out_buf, gate_buf, up_buf, down_buf)
    dp = lax.axis_index("dp")
    z = lax.axis_index("mp")
    core = lax.rem(dp, 2)
    x = lax.rem(dp // 2, 2)
    y = dp // 4
    up_z = lax.rem(z + 1, ring)
    down_z = lax.rem(z + ring - 1, ring)
    whole = slice(None)
    to_x = {"dp": (y * 2 + 1 - x) * 2 + core, "mp": z}
    to_y = {"dp": ((1 - y) * 2 + x) * 2 + core, "mp": z}
    to_core = {"dp": (y * 2 + x) * 2 + 1 - core, "mp": z}
    to_up = {"dp": dp, "mp": up_z}
    to_down = {"dp": dp, "mp": down_z}
    steps = ring - 1
    first_pair, second_pair, across = 2 * steps, 2 * steps + 1, 2 * steps + 2
    hops = 2 * steps + 3

    def x_leads(which, piece):
        return (which + piece) % 2 == 0

    def z_leads(piece):
        return piece < PIECES - 1

    def target(which, piece, hop):
        if hop < steps:
            return to_up
        if hop < 2 * steps:
            return to_down
        if hop == across:
            return to_core
        return to_x if (hop == first_pair) == x_leads(which, piece) else to_y

    def region(which, piece, hop):
        pair = (y, whole) if x_leads(which, piece) else (whole, x)
        if hop == across:
            return (whole, whole, core, whole)
        if hop == first_pair:
            return (y, x, core, whole if z_leads(piece) else z)
        if hop == second_pair:
            return pair + (core, whole if z_leads(piece) else z)
        block = z - hop if hop < steps else z + (hop - steps)
        return ((y, x) if z_leads(piece) else (whole, whole)) + (core, block)

    def sends_now(hop):
        if hop < steps:
            return jnp.logical_and(z >= hop, z < ring - 1)
        return jnp.logical_and(z + (hop - steps) < ring, z > 0)

    def lands_now(hop):
        if hop < steps:
            return z >= hop + 1
        return z + (hop - steps) + 1 < ring

    def copy(which, piece, hop, fixed=False):
        at = region(which, piece, hop)
        if fixed and hop < 2 * steps:
            at = at[:3] + (z,)
        part = bufs[which].at[at + (whole, piece)]
        slot = (which * PIECES + piece) * hops + hop
        return pltpu.make_async_remote_copy(
            src_ref=part, dst_ref=part, send_sem=send_sem.at[slot], recv_sem=recv_sem.at[slot],
            device_id=target(which, piece, hop), device_id_type=MESH,
        )

    def guarded(hop, condition, action):
        if hop < 2 * steps:
            pl.when(condition(hop))(action)
        else:
            action()

    def send(which, piece, hop):
        guarded(hop, sends_now, lambda: copy(which, piece, hop).start())

    def land(which, piece, hop):
        guarded(hop, lands_now, lambda: copy(which, piece, hop, True).wait_recv())

    def sent(which, piece, hop):
        guarded(hop, sends_now, lambda: copy(which, piece, hop, True).wait_send())

    def own(which):
        source = (qkv_in, out_in, ffn_in.at[pl.ds(0, 1)], ffn_in.at[pl.ds(1, 1)], down_in)[which]
        return pltpu.make_async_copy(source, bufs[which].at[y, x, core, z], local_sem.at[which])

    line = [((), (0, steps))]
    for step in range(1, steps):
        line.append(((step - 1, steps + step - 1), (step, steps + step)))
    line_end = (steps - 1, 2 * steps - 1)
    z_first = line + [
        (line_end, (first_pair,)), ((first_pair,), (second_pair,)), ((second_pair,), (across,)),
        ((across,), ()),
    ]
    z_last = [((), (first_pair,)), ((first_pair,), (second_pair,)), ((second_pair,), line[0][1])]
    z_last += line[1:] + [(line_end, (across,)), ((across,), ())]

    def event(which, stage, late):
        for piece in range(PIECES):
            if z_leads(piece) == bool(late):
                continue
            waits, sends = (z_first if z_leads(piece) else z_last)[stage]
            for hop in waits:
                land(which, piece, hop)
            for hop in sends:
                send(which, piece, hop)

    order = event_order(len(bufs))
    cursor = [0]

    def take(count):
        picked = order[cursor[0]:cursor[0] + count]
        cursor[0] += len(picked)
        return picked

    def until(which):
        ends = [order.index((which, STAGES - 1, late)) for late in range(2)]
        return take(max(ends) + 1 - cursor[0])

    def at_steps(total, picked):
        plan = [[] for _ in range(total)]
        for place, item in enumerate(picked):
            plan[place * total // len(picked)].append(item)

        def run(step):
            for place, items in enumerate(plan):
                if items:
                    @pl.when(step == place)
                    def _():
                        for item in items:
                            event(*item)
        return run

    for which in range(len(bufs)):
        own(which).start()
    barrier = pltpu.get_barrier_semaphore()
    for peer in (to_x, to_y, to_core, to_up, to_down):
        pl.semaphore_signal(barrier, inc=1, device_id=peer, device_id_type=MESH)
    pl.semaphore_wait(barrier, 5)
    for which in range(len(bufs)):
        own(which).wait()

    first_wave = until(0)
    cut = min(3, len(first_wave))
    for item in first_wave[:cut]:
        event(*item)

    total_rows, width = tokens_ref.shape
    blocks = total_rows // ROWS

    def norm_rows(source, gain_row):
        gain = gain_ref[gain_row:gain_row + 1, :]

        def body(step, carry):
            rows = pl.ds(pl.multiple_of(step * 128, 128), 128)
            wide = source[rows, :].astype(jnp.float32)
            square = jnp.mean(wide * wide, axis=-1, keepdims=True)
            normed[rows, :] = (wide * lax.rsqrt(square + 1e-05) * gain).astype(jnp.bfloat16)
            return carry
        lax.fori_loop(0, total_rows // 128, body, 0)

    norm_rows(tokens_ref, 0)
    ids = ids_ref[...].astype(jnp.float32)
    times = jnp.broadcast_to(ids[2:3, :], (WIDE, total_rows)).T
    columns[0] = jnp.broadcast_to(ids[0:1, :], (WIDE, total_rows)).T
    columns[1] = jnp.broadcast_to(ids[1:2, :], (WIDE, total_rows)).T
    half = HEAD_DIM // 2
    lane = lax.broadcasted_iota(jnp.int32, (1, WIDE), 1)
    slot_in_half = lax.rem(lane, half).astype(jnp.float32)
    freq = jnp.exp(slot_in_half * (-math.log(10000.0) / half))
    front = lax.rem(lane, HEAD_DIM) < half
    angle = times * freq
    cosine[...] = jnp.cos(angle)
    sine[...] = jnp.where(front, -1.0, 1.0) * jnp.sin(angle)

    for item in first_wave[cut:]:
        event(*item)

    def rotated_wide(raw):
        swapped = jnp.where(front, pltpu.roll(raw, WIDE - half, 1), pltpu.roll(raw, half, 1))
        return raw * cosine[...] + swapped * sine[...]

    later = until(2)
    early_count = min(len(later), 3)
    project_events = at_steps(ring, later[:early_count])
    attend_steps = (width // WIDE) * blocks
    attend_events = at_steps(attend_steps, later[early_count:])

    def project(step, carry):
        def product(kind):
            shape = (width, qkv_buf.shape[-1])
            weight = qkv_buf[:, :, :, step, kind].reshape(shape)
            return jnp.dot(normed[...], weight, preferred_element_type=jnp.float32)
        groups = qkv_buf.shape[-1] // WIDE
        for kind, held in enumerate((queries, keys, values)):
            raw = product(kind)
            for group in range(groups):
                part = raw[:, group * WIDE:(group + 1) * WIDE]
                if kind < 2:
                    part = rotated_wide(part)
                part = part.astype(jnp.bfloat16)
                if kind == 0:
                    part = part * jnp.bfloat16(HEAD_DIM ** -0.5)
                held[step * groups + group] = part
        project_events(step)
        return carry
    lax.fori_loop(0, ring, project, 0)

    left = lane < HEAD_DIM

    def attend_step(step, carry):
        pair = step // blocks
        block = lax.rem(step, blocks)
        rows = pl.ds(pl.multiple_of(block * ROWS, ROWS), ROWS)
        base = pl.multiple_of((block * ROWS) // L * L, L)
        span = pl.ds(base, L)
        same_series = columns[0, rows, 0:1] == ids_ref[0:1, span].astype(jnp.float32)
        same_variate = columns[1, rows, 0:1] == ids_ref[1:2, span].astype(jnp.float32)
        both = queries[pair, rows, :]
        key_rows = keys[pair, span, :]
        value_rows = values[pair, span, :]
        results = []
        for side in range(2):
            head = pair * 2 + side
            chosen = left if side == 0 else jnp.logical_not(left)
            mine = both * chosen.astype(jnp.bfloat16)
            scores = lax.dot_general(
                mine, key_rows, (((1,), (1,)), ((), ())), preferred_element_type=jnp.float32
            )
            scores = scores + jnp.where(same_variate, bias_ref[0, head], bias_ref[1, head])
            scores = jnp.where(same_series, scores, -1e30)
            top = jnp.max(scores, axis=1, keepdims=True)
            expo = jnp.exp(scores - top)
            total = jnp.sum(expo, axis=1, keepdims=True)
            mixed = jnp.dot(
                expo.astype(jnp.bfloat16), value_rows, preferred_element_type=jnp.float32
            )
            results.append(mixed / total)
        lanes = pl.ds(pl.multiple_of(pair * WIDE, WIDE), WIDE)
        attended[rows, lanes] = jnp.where(left, results[0], results[1]).astype(jnp.bfloat16)
        attend_events(step)
        return carry
    lax.fori_loop(0, attend_steps, attend_step, 0)

    def block_pair(buf, side_y, side_x, index):
        return jnp.concatenate(
            [buf[side_y, side_x, half_core, index].reshape(-1, buf.shape[-1]) for half_core in range(2)],
            axis=1,
        )

    slab = 2 * out_buf.shape[-1]

    def out_step(step, carry):
        lanes = pl.ds(pl.multiple_of(step * slab, slab), slab)
        weight = block_pair(out_buf, step // 2, lax.rem(step, 2), whole)
        mixed = jnp.dot(attended[...], weight, preferred_element_type=jnp.float32)
        residual[:, lanes] = (tokens_ref[:, lanes].astype(jnp.float32) + mixed).astype(jnp.bfloat16)
        return carry
    lax.fori_loop(0, 4, out_step, 0)
    norm_rows(residual, 1)

    gate_events = at_steps(ring, until(3))

    def gate_step(step, carry):
        weight = gate_buf[:, :, :, step].reshape(width, gate_buf.shape[-1])
        gates[step] = jnp.dot(normed[...], weight, preferred_element_type=jnp.float32)
        gate_events(step)
        return carry
    lax.fori_loop(0, ring, gate_step, 0)

    up_events = at_steps(ring, until(4))

    def up_step(step, carry):
        weight = up_buf[:, :, :, step].reshape(width, up_buf.shape[-1])
        up = jnp.dot(normed[...], weight, preferred_element_type=jnp.float32)
        gate = gates[step]
        hidden[step] = (gate / (1.0 + jnp.exp(-gate)) * up).astype(jnp.bfloat16)
        up_events(step)
        return carry
    lax.fori_loop(0, ring, up_step, 0)

    def down_step(step, carry):
        lanes = pl.ds(pl.multiple_of(step * slab, slab), slab)
        total = residual[:, lanes].astype(jnp.float32)
        for index in range(ring):
            weight = block_pair(down_buf, step // 2, lax.rem(step, 2), index)
            total = total + jnp.dot(hidden[index], weight, preferred_element_type=jnp.float32)
        final_ref[:, lanes] = total.astype(jnp.bfloat16)
        return carry
    lax.fori_loop(0, 4, down_step, 0)

    for which in range(len(bufs)):
        for piece in range(PIECES):
            for hop in range(hops):
                sent(which, piece, hop)


def fused(
    ring, tokens, norm_gain, qkv_weight, out_weight, variate_bias, ffn_weight, down_weight,
    sample_ids, variate_ids, time_ids,
):
    rows, width = tokens.shape
    ids = jnp.stack([sample_ids, variate_ids, time_ids])
    qkv = qkv_weight.reshape(qkv_weight.shape[0], PIECES, -1, qkv_weight.shape[2])
    out = out_weight.reshape(1, PIECES, -1, out_weight.shape[1])
    ffn = ffn_weight.reshape(2, PIECES, -1, ffn_weight.shape[2])
    down = down_weight.reshape(1, PIECES, -1, down_weight.shape[1])
    shapes = (qkv.shape, out.shape, (1,) + ffn.shape[1:], (1,) + ffn.shape[1:], down.shape)
    buffers = [pltpu.VMEM((2, 2, 2, ring) + shape, jnp.bfloat16) for shape in shapes]
    pairs = width // WIDE
    per_pair = pltpu.VMEM((pairs, rows, WIDE), jnp.bfloat16)
    flat = pltpu.VMEM((rows, width), jnp.bfloat16)
    vmem = pl.BlockSpec(memory_space=pltpu.VMEM)
    anywhere = pl.BlockSpec(memory_space=pl.ANY)
    copies = len(shapes) * PIECES * (2 * ring + 1)
    return pl.pallas_call(
        functools.partial(layer_kernel, ring),
        out_shape=jax.ShapeDtypeStruct((rows, width), jnp.bfloat16),
        in_specs=[pl.BlockSpec(memory_space=pltpu.SMEM), vmem, vmem, vmem] + [anywhere] * 4,
        out_specs=vmem,
        scratch_shapes=buffers + [
            flat, per_pair, per_pair, per_pair, flat, flat,
            pltpu.VMEM((ring, rows, ffn.shape[-1]), jnp.float32),
            pltpu.VMEM((ring, rows, ffn.shape[-1]), jnp.bfloat16),
            pltpu.VMEM((rows, WIDE), jnp.float32),
            pltpu.VMEM((rows, WIDE), jnp.float32),
            pltpu.VMEM((2, rows, WIDE), jnp.float32),
            pltpu.SemaphoreType.DMA((copies,)),
            pltpu.SemaphoreType.DMA((copies,)),
            pltpu.SemaphoreType.DMA((len(shapes),)),
        ],
        compiler_params=pltpu.CompilerParams(
            collective_id=0, has_side_effects=True, vmem_limit_bytes=60 * 1024 * 1024
        ),
    )(variate_bias, tokens, norm_gain, ids, qkv, out, ffn, down)


def solution(mesh):
    ring = mesh.shape["mp"]
    body = functools.partial(fused, ring) if (mesh.shape["dp"], ring) == (2 ** 3, 2 ** 2) else local
    return jax.shard_map(
        body,
        mesh=mesh,
        in_specs=(
            P(("dp", "mp"), None),
            P(),
            P(None, "dp", "mp"),
            P("mp", "dp"),
            P(),
            P(None, "dp", "mp"),
            P("mp", "dp"),
            P(("dp", "mp")),
            P(("dp", "mp")),
            P(("dp", "mp")),
        ),
        out_specs=P(("dp", "mp"), None),
        check_vma=False,
    )
```
